256 devices in a mesh: parts: 2 (over y), expert: 16 (over z), tensor: 4 (over x), seq: 2 (over core).
Axes of the slice: x: 4, y: 2, z: 16, core: 2. Of those that a mesh axis runs over, the one named last changes fastest.
The devices are a block of a 4x16x16 slice.
Arguments:
- tokens: bfloat16 [1024, 4096], P(('parts', 'expert', 'tensor', 'seq')), parts along dimension 0, may hold values from -6 to 6
- out_grad: bfloat16 [1024, 4096], P(('parts', 'expert', 'tensor', 'seq')), parts along dimension 0, may hold values from -3 to 3
- expert_ids: int32 [1024, 2], P(('parts', 'expert', 'tensor', 'seq')), parts along dimension 0, may hold values from 0 to 3, all different within a row; in each aligned block of 4 rows (0 to 3, 4 to 7, ...) at most 3 rows name the same one
- probs: bfloat16 [1024, 2], P(('parts', 'expert', 'tensor', 'seq')), parts along dimension 0, may hold values from 0.19921875 to 1
- w_gate: bfloat16 [16, 4096, 2048], P('expert', None, ('tensor', 'seq')), may hold values from -0.09375 to 0.09375
- w_up: bfloat16 [16, 4096, 2048], P('expert', None, ('tensor', 'seq')), may hold values from -0.09375 to 0.09375
- w_down: bfloat16 [16, 2048, 4096], P('expert', ('tensor', 'seq')), may hold values from -0.0625 to 0.0625
Outputs:
- grad_tokens: float32 [1024, 4096], P(('parts', 'expert', 'tensor', 'seq')), parts along dimension 0
- grad_probs: float32 [1024, 2], P(('parts', 'expert', 'tensor', 'seq')), parts along dimension 0
- grad_gate: bfloat16 [32, 4096, 2048], P(('parts', 'expert'), None, ('tensor', 'seq')), parts along dimension 0
- grad_up: bfloat16 [32, 4096, 2048], P(('parts', 'expert'), None, ('tensor', 'seq')), parts along dimension 0
- grad_down: bfloat16 [32, 2048, 4096], P(('parts', 'expert'), ('tensor', 'seq')), parts along dimension 0
The draws below stay inside these ranges and needn't reach their ends.
There are 2 independent parts, one for each index of `parts`. The reference program is written for one: setup_inputs(seed, part) draws one part's arguments, and reference() takes and returns one part's arrays. A program takes and returns all parts, laid end to end along the dimension named above; an argument that names none is the same for every part. Nothing has to cross between parts.
Inputs may be any that keep to these rules, and one draw needn't show every extreme that they name: `expert_ids`: each row names 2 different experts. Within the rows of one device (aligned blocks of 4 rows) no expert is named by more than 3 rows, a bound that some block reaches.
All inputs are finite; a program needn't handle non-finite values.
Results may differ from the reference program's by a relative error of at most 0.005.
Values may be sent and summed in bfloat16 or wider, within the bound.
A program may use at most 128 MiB of HBM per device.

```python
import math
import jax
import jax.numpy as jnp
import numpy as np
from jax import lax

D = 4096
FFW = 8192
EXPERTS = 4
TOP = 2
TOK_DEV = 4
CAP = 3
SPLIT = 4
TOKENS = 512
N_EXPERT = 16


def shard_levels(rng, dims, cuts, least, largest):
    level = 1.0
    for dim, blocks in cuts:
        steps = jax.random.uniform(jax.random.fold_in(jax.random.fold_in(rng, 6), dim), (blocks,), jnp.float32, least / len(cuts), largest / len(cuts))
        level = level * jnp.repeat(jnp.exp(steps), dims[dim] // blocks).reshape((-1,) + (1,) * (len(dims) - 1 - dim))
    return level


def deal_out(stream_key, own, number, rows, number_of, top, reach, skew):
    sequence = jax.random.permutation(stream_key, number_of)
    packed, ordinary = portions_of(number_of, rows * top, reach, skew, True), portions_of(number_of, rows * top, reach, skew, False)
    places = jnp.arange(number_of)

    def named(tallies, offset_by):
        used = int((tallies > 0).sum())
        fixed = max(1, used // 4)
        moved = fixed + (places - fixed + offset_by * (used - fixed)) % max(1, number_of - fixed)
        return jnp.zeros((number_of,), jnp.int32).at[sequence[jnp.where(places < fixed, places, moved)]].set(jnp.asarray(tallies, jnp.int32))

    tallies = jnp.where(number % 4 == 0, named(packed, number // 4), named(ordinary, number - number // 4 - 1))
    mixed = jax.random.permutation(jax.random.fold_in(own, 3), number_of)
    source_of, sink = mixed[0:number_of // 2 * 2:2], mixed[1:number_of // 2 * 2:2]
    margin = jnp.minimum(tallies[source_of] - 1, reach - tallies[sink]) // 2
    margin = jnp.where((source_of == sequence[0]) | (sink == sequence[0]) | (tallies[sink] == 0), 0, jnp.maximum(margin, 0))
    moved = jax.random.randint(jax.random.fold_in(own, 4), (number_of // 2,), 0, 1 << 20) % (margin + 1)
    tallies = tallies.at[source_of].add(-moved).at[sink].add(moved)
    items = jnp.searchsorted(jnp.cumsum(tallies), jnp.arange(rows * top), side="right").astype(jnp.int32)
    table = items.reshape(top, rows).T
    table = table[jax.random.permutation(jax.random.fold_in(own, 1), rows)]
    offset_by = jax.random.randint(jax.random.fold_in(own, 2), (rows, 1), 0, top)
    return jnp.take_along_axis(table, (jnp.arange(top)[None, :] + offset_by) % top, axis=1)


def portions_of(count, total, limit, lean, full):
    portions = [(1 << 20) // math.isqrt(standing ** lean) + 1 for standing in range(1, count + 1)]
    largest = limit if full else min(limit, max(-(-total // count), total * portions[0] // sum(portions)))
    least = 1 if total - largest >= count - 1 else 0
    counts, rest = [largest] + [least] * (count - 1), total - largest - least * (count - 1)
    while rest > 0:
        movable = [i for i in range(1, count) if counts[i] < largest] or [i for i in range(1, count) if counts[i] < limit]
        pool, budget = sum([portions[i] for i in movable]), rest
        for i in movable:
            more = min(limit - counts[i], max(1, budget * portions[i] // pool), rest)
            counts[i] = counts[i] + more
            rest = rest - more
    return np.array(counts)


def centred(key, dims, deviation, bound, cuts=(), kind=jnp.bfloat16):
    gain = shard_levels(key, dims, cuts, -0.22, 0.18) if cuts else 1.0
    drawn = jax.random.normal(key, dims, jnp.float32) * deviation * gain
    return jnp.minimum(jnp.maximum(drawn, -bound), bound).astype(kind)


def setup_inputs(seed: int = 0, part: int = 0) -> dict:
    key_of = jax.random.split(jax.random.key(seed), 8)
    part_splits = jax.random.split(jax.random.fold_in(key_of[7], part), 8)
    tokens = centred(part_splits[0], (TOKENS, D), 1.0, 6.0, ((0, 128),))
    out_grad = centred(part_splits[1], (TOKENS, D), 0.5, 3.0, ((0, 128),))
    expert_ids_keys = jax.random.split(jax.random.fold_in(part_splits[2], 1), TOKENS // TOK_DEV)
    expert_ids_turns = jax.random.permutation(jax.random.fold_in(part_splits[2], 3), TOKENS // TOK_DEV)
    expert_ids = jax.vmap(lambda own, number: deal_out(jax.random.fold_in(part_splits[2], 2), own, number, TOK_DEV, EXPERTS, TOP, CAP, 2))(expert_ids_keys, expert_ids_turns).reshape((TOKENS, TOP))
    probs = jnp.clip(0.19921875 + 0.80078125 * jax.random.uniform(part_splits[3], (TOKENS, TOP), jnp.float32) ** shard_levels(part_splits[3], (TOKENS, TOP), ((0, 128),), -0.2, 0.2), 0.19921875, 1.0).astype(jnp.bfloat16)
    w_gate = centred(key_of[4], (N_EXPERT, D, FFW // SPLIT), D ** -0.5, 0.09375, ((0, 16), (2, 8)))
    w_up = centred(key_of[5], (N_EXPERT, D, FFW // SPLIT), D ** -0.5, 0.09375, ((0, 16), (2, 8)))
    w_down = centred(key_of[6], (N_EXPERT, FFW // SPLIT, D), FFW ** -0.5, 0.0625, ((0, 16), (1, 8)))
    return {"tokens": tokens, "out_grad": out_grad, "expert_ids": expert_ids, "probs": probs, "w_gate": w_gate, "w_up": w_up, "w_down": w_down}


def silu_parts(gate):
    sigma = jax.nn.sigmoid(gate)
    return gate * sigma, sigma * (1.0 + gate * (1.0 - sigma))


def reference(tokens, out_grad, expert_ids, probs, w_gate, w_up, w_down):
    total = tokens.shape[0]
    sources = total // TOK_DEV
    split = N_EXPERT // EXPERTS
    local = FFW // split
    ids = expert_ids.reshape(sources, TOK_DEV * TOP)
    onehot = (ids[:, :, None] == jnp.arange(EXPERTS, dtype=jnp.int32)[None, None, :]).astype(jnp.int32)
    before = jnp.cumsum(onehot, axis=1) - onehot
    slot = jnp.sum(before * onehot, axis=2)
    anchor = jnp.arange(sources, dtype=jnp.int32)[:, None]
    place = ((ids * sources + anchor) * CAP + slot).reshape(-1).astype(jnp.int32)
    rows_total = EXPERTS * sources * CAP
    owner_token = (jnp.arange(total * TOP, dtype=jnp.int32) // TOP).astype(jnp.int32)
    table = jnp.full((rows_total,), total, jnp.int32).at[place].set(owner_token)
    scales = jnp.zeros((rows_total,), jnp.float32).at[place].set(probs.reshape(-1).astype(jnp.float32))
    padded_x = jnp.concatenate([tokens, jnp.zeros((1, D), tokens.dtype)], axis=0)
    padded_dy = jnp.concatenate([out_grad, jnp.zeros((1, D), out_grad.dtype)], axis=0)
    gate_full = w_gate.reshape(EXPERTS, split, D, local).transpose(0, 2, 1, 3).reshape(EXPERTS, D, FFW)
    up_full = w_up.reshape(EXPERTS, split, D, local).transpose(0, 2, 1, 3).reshape(EXPERTS, D, FFW)
    down_full = w_down.reshape(EXPERTS, FFW, D)

    def one_expert(inputs):
        index, scale, w_g, w_u, w_d = inputs
        rows_x = padded_x[index]
        rows_dy = padded_dy[index]
        scale = scale[:, None]
        gate = jnp.dot(rows_x, w_g, preferred_element_type=jnp.float32)
        up = jnp.dot(rows_x, w_u, preferred_element_type=jnp.float32)
        back = lax.dot_general(rows_dy, w_d, (((1,), (1,)), ((), ())), preferred_element_type=jnp.float32)
        act, slope = silu_parts(gate)
        hidden = act * up
        score = jnp.sum(back * hidden, axis=1)
        scaled = scale * back
        d_gate = (scaled * up * slope).astype(jnp.bfloat16)
        d_up = (scaled * act).astype(jnp.bfloat16)
        weighted = (scale * hidden).astype(jnp.bfloat16)
        part_dx = lax.dot_general(d_gate, w_g, (((1,), (1,)), ((), ())), preferred_element_type=jnp.float32)
        part_dx = part_dx + lax.dot_general(d_up, w_u, (((1,), (1,)), ((), ())), preferred_element_type=jnp.float32)
        sum_g = lax.dot_general(rows_x, d_gate, (((0,), (0,)), ((), ())), preferred_element_type=jnp.float32)
        sum_u = lax.dot_general(rows_x, d_up, (((0,), (0,)), ((), ())), preferred_element_type=jnp.float32)
        sum_d = lax.dot_general(weighted, rows_dy, (((0,), (0,)), ((), ())), preferred_element_type=jnp.float32)
        return part_dx, score, sum_g.astype(jnp.bfloat16), sum_u.astype(jnp.bfloat16), sum_d.astype(jnp.bfloat16)

    inputs = (table.reshape(EXPERTS, sources * CAP), scales.reshape(EXPERTS, sources * CAP), gate_full, up_full, down_full)
    part_dx, score, grad_g, grad_u, grad_d = lax.map(one_expert, inputs)
    flat_dx = part_dx.reshape(rows_total, D)
    flat_score = score.reshape(rows_total)
    grad_tokens = jnp.sum(flat_dx[place].reshape(total, TOP, D), axis=1)
    grad_probs = flat_score[place].reshape(total, TOP)
    grad_gate = grad_g.reshape(EXPERTS, D, split, local).transpose(0, 2, 1, 3).reshape(N_EXPERT, D, local)
    grad_up = grad_u.reshape(EXPERTS, D, split, local).transpose(0, 2, 1, 3).reshape(N_EXPERT, D, local)
    grad_down = grad_d.reshape(N_EXPERT, local, D)
    return (grad_tokens, grad_probs, grad_gate, grad_up, grad_down)
```

```python
import functools
import jax
import jax.numpy as jnp
from jax import lax
from jax.experimental import pallas as pl
from jax.experimental.pallas import tpu as pltpu
from jax.sharding import PartitionSpec as P

EXPERTS = 4
TOP = 2
LANES = 128
MESH = pl.DeviceIdType.MESH


def places():
    z, x, c = lax.axis_index("expert"), lax.axis_index("tensor"), lax.axis_index("seq")
    ring, line = lax.axis_size("expert"), lax.axis_size("tensor")
    along_z = ({"expert": lax.rem(z + 1, ring)}, {"expert": lax.rem(z + ring - 1, ring)})
    along_x = ({"tensor": lax.rem(x + 1, line)}, {"tensor": lax.rem(x + line - 1, line)})
    return z, x, c, along_z, along_x, {"seq": 1 - c}


def greet(devices):
    barrier = pltpu.get_barrier_semaphore()
    for device in devices:
        pl.semaphore_signal(barrier, inc=1, device_id=device, device_id_type=MESH)
    pl.semaphore_wait(barrier, len(devices))


class Wires:
    def __init__(self, send_sem, recv_sem):
        self.send_sem, self.recv_sem, self.at, self.sent = send_sem, recv_sem, {}, []

    def copy(self, name, src, dst, device):
        k = self.at.setdefault(name, len(self.at))
        return pltpu.make_async_remote_copy(
            src_ref=src,
            dst_ref=dst,
            send_sem=self.send_sem.at[k],
            recv_sem=self.recv_sem.at[k],
            device_id=device,
            device_id_type=MESH,
        )

    def send(self, name, src, dst, device):
        copy = self.copy(name, src, dst, device)
        copy.start()
        self.sent.append(copy)

    def arrived(self, name, ref, device):
        self.copy(name, ref, ref, device).wait_recv()

    def drain(self):
        for copy in self.sent:
            copy.wait_send()


def split_score(score):
    high = score.astype(jnp.bfloat16)
    rest = (score - high.astype(jnp.float32)).astype(jnp.bfloat16)
    lanes = lax.broadcasted_iota(jnp.int32, score.shape, score.ndim - 1)
    return jnp.where(lanes < LANES // 2, high.astype(jnp.float32), rest.astype(jnp.float32))


def joined_score(block):
    return block + pltpu.roll(block, LANES // 2, 1)


def pack(rows):
    score = split_score(joined_score(rows[:, -LANES:]))
    return jnp.concatenate([rows[:, :-LANES], score], axis=1).astype(jnp.bfloat16)


def cut(columns):
    first = columns // 2 // LANES * LANES
    return ((0, first), (first, columns - first))


def gather_kernel(xy_ref, x_out, dy_out, table_out, inc, buf_a, buf_b, send_sem, recv_sem, out_sem):
    z, x, c, along_z, along_x, partner = places()
    ring, line = buf_a.shape[1], buf_a.shape[2]
    half = ring // 2
    wide, narrow = buf_a.shape[-1], buf_b.shape[-1]
    cut_a, cut_b = cut(wide), cut(narrow)
    wires = Wires(send_sem, recv_sem)
    greet((partner, *along_z, *along_x))

    def slabs(k):
        if k == 0:
            return (z,)
        if k == half:
            return (lax.rem(z + half, ring),)
        return (lax.rem(z + ring - k, ring), lax.rem(z + k, ring))

    def block(s, y):
        return buf_a.at[c, s, lax.rem(y + line, line)]

    def part(s, y, d):
        return buf_a.at[c, s, lax.rem(y + line, line), :, pl.ds(*cut_a[d])]

    def to_x(s, key):
        for d in (0, 1):
            wires.send(("x", d, key), block(s, x), block(s, x), along_x[d])

    def x_on(s, key):
        for d, y in ((0, x - 1), (1, x + 1)):
            wires.arrived(("x", d, key), block(s, y), along_x[d])
            wires.send(("h", d, key), part(s, y, d), part(s, y, d), along_x[d])

    def x_end(s, key):
        for d in (0, 1):
            wires.arrived(("h", d, key), part(s, x + 2, d), along_x[d])
        wires.send(("da", key), buf_a.at[c, s], buf_a.at[c, s], partner)

    def b_part(s, d):
        return buf_b.at[c, s, :, :, pl.ds(*cut_b[d])]

    def to_z(s, d, k):
        if k < half:
            wires.send(("za", d, k), block(s, x), block(s, x), along_z[d])
        else:
            wires.send(("za", d, k), part(s, x, d), part(s, x, d), along_z[d])

    def to_z_b(s, d, k):
        ref = buf_b.at[c, s] if k < half else b_part(s, d)
        wires.send(("zb", d, k), ref, ref, along_z[d])

    wires.send("pair", xy_ref.at[1 - c], inc, partner)
    wires.arrived("pair", inc, partner)
    merged = xy_ref[c] + inc[...]
    buf_a[c, z, x] = merged[:, :wide]
    buf_b[c, z, x] = merged[:, wide:]

    def narrow_block(y):
        return buf_b.at[c, z, lax.rem(y + line, line)]

    def narrow_part(y, d):
        return buf_b.at[c, z, lax.rem(y + line, line), :, pl.ds(*cut_b[d])]

    for d in (0, 1):
        wires.send(("b", d), narrow_block(x), narrow_block(x), along_x[d])
    for d in (0, 1):
        to_z(z, d, 1)
    to_x(z, (0, 0))
    for d, y in ((0, x - 1), (1, x + 1)):
        wires.arrived(("b", d), narrow_block(y), along_x[d])
        wires.send(("bh", d), narrow_part(y, d), narrow_part(y, d), along_x[d])
    for d in (0, 1):
        wires.arrived(("bh", d), narrow_part(x + 2, d), along_x[d])
    for d in (0, 1):
        to_z_b(z, d, 1)
    wires.send(("db", (0, 0)), buf_b.at[c, z], buf_b.at[c, z], partner)

    for k in range(1, half + 3):
        if k < half:
            for d, s in enumerate(slabs(k)):
                wires.arrived(("za", d, k), block(s, x), along_z[d])
                to_z(s, d, k + 1)
                to_x(s, (k, d))
            for d, s in enumerate(slabs(k)):
                wires.arrived(("zb", d, k), buf_b.at[c, s], along_z[d])
                to_z_b(s, d, k + 1)
                wires.send(("db", (k, d)), buf_b.at[c, s], buf_b.at[c, s], partner)
        elif k == half:
            (s,) = slabs(k)
            for d in (0, 1):
                wires.arrived(("za", d, k), part(s, x, d), along_z[d])
            to_x(s, (k, 0))
            for d in (0, 1):
                wires.arrived(("zb", d, k), b_part(s, d), along_z[d])
            wires.send(("db", (k, 0)), buf_b.at[c, s], buf_b.at[c, s], partner)
        if 0 <= k - 1 <= half:
            for d, s in enumerate(slabs(k - 1)):
                x_on(s, (k - 1, d))
        if 0 <= k - 2 <= half:
            for d, s in enumerate(slabs(k - 2)):
                x_end(s, (k - 2, d))

    for k in range(half + 1):
        for d, s in enumerate(slabs(k)):
            wires.arrived(("da", (k, d)), buf_a.at[1 - c, s], partner)
            wires.arrived(("db", (k, d)), buf_b.at[1 - c, s], partner)
    width = x_out.shape[-1]
    head = wide - LANES
    outs = []
    for m, out in ((0, x_out), (1, dy_out)):
        outs.append((buf_a.at[m, :, :, :, pl.ds(0, head)], out.at[:, :, :, pl.ds(0, head)]))
        outs.append((buf_b.at[m], out.at[:, :, :, pl.ds(head, narrow)]))
    outs.append((buf_a.at[1, :, :, :, pl.ds(head, LANES)], table_out))
    copies = [pltpu.make_async_copy(a, b, out_sem.at[i]) for i, (a, b) in enumerate(outs)]
    for copy in copies:
        copy.start()
    wires.drain()
    for copy in copies:
        copy.wait()


def gather_rows(xy, wide):
    ring, line = lax.axis_size("expert"), lax.axis_size("tensor")
    rows, columns = xy.shape[1:]
    width = columns - LANES
    narrow = columns - wide
    half = ring // 2
    wires = 1 + 4 + 4 * half + 4 * ring + 2 * ring
    whole = jax.ShapeDtypeStruct((ring, line, rows, width), xy.dtype)
    return pl.pallas_call(
        gather_kernel,
        out_shape=(whole, whole, jax.ShapeDtypeStruct((ring, line, rows, LANES), xy.dtype)),
        in_specs=[pl.BlockSpec(memory_space=pltpu.VMEM)],
        out_specs=(pl.BlockSpec(memory_space=pl.ANY),) * 3,
        scratch_shapes=[
            pltpu.VMEM((rows, columns), xy.dtype),
            pltpu.VMEM((2, ring, line, rows, wide), xy.dtype),
            pltpu.VMEM((2, ring, line, rows, narrow), xy.dtype),
            pltpu.SemaphoreType.DMA((wires,)),
            pltpu.SemaphoreType.DMA((wires,)),
            pltpu.SemaphoreType.DMA((5,)),
        ],
        compiler_params=pltpu.CompilerParams(collective_id=0, has_side_effects=True),
        name="gather_rows",
    )(xy)


def reduce_kernel(part_ref, out_ref, other, mid, mid_in, full, full_in, zs, zs_in, send_sem, recv_sem):
    z, x, c, along_z, along_x, partner = places()
    ring, line = part_ref.shape[1], part_ref.shape[2]
    half = ring // 2
    width = part_ref.shape[-1]
    cuts = cut(width)
    wires = Wires(send_sem, recv_sem)
    greet((partner, *along_z, *along_x))

    def slabs(k):
        if k == 0:
            return (z,)
        if k == half:
            return (lax.rem(z + half, ring),)
        return (lax.rem(z + k, ring), lax.rem(z + ring - k, ring))

    keys = [(k, d) for k in range(half, -1, -1) for d in range(1 if k in (0, half) else 2)]
    slot = {key: i for i, key in enumerate(keys)}

    def chip_sum(s, y):
        y = lax.rem(y + line, line)
        return part_ref[c, s, y].astype(jnp.float32) + other[s, y].astype(jnp.float32)

    def with_part(rows, ref, i, d):
        lo, n = cuts[d]
        added = rows[:, lo : lo + n] + ref[i, :, pl.ds(lo, n)].astype(jnp.float32)
        pieces = [added, rows[:, n:]] if d == 0 else [rows[:, :lo], added]
        return jnp.concatenate(pieces, axis=1)

    def start_x(s, key):
        wires.arrived(("d", key), other.at[s], partner)
        i = slot[key]
        mid[i] = pack(chip_sum(s, x + 2))
        for d, device in ((0, along_x[1]), (1, along_x[0])):
            at = pl.ds(*cuts[d])
            wires.send(("h", d, key), mid.at[i, :, at], mid_in.at[i, :, at], device)

    def middle_x(s, key):
        i = slot[key]
        for d, y, device in ((0, x - 1, along_x[1]), (1, x + 1, along_x[0])):
            wires.arrived(("h", d, key), mid_in.at[i, :, pl.ds(*cuts[d])], device)
            full[d, i] = pack(with_part(chip_sum(s, y), mid_in, i, d))
            wires.send(("f", d, key), full.at[d, i], full_in.at[d, i], device)

    def end_x(s, key):
        i = slot[key]
        for d, device in ((0, along_x[1]), (1, along_x[0])):
            wires.arrived(("f", d, key), full_in.at[d, i], device)
        total = chip_sum(s, x)
        return total + full_in[0, i].astype(jnp.float32) + full_in[1, i].astype(jnp.float32)

    def hop_z(total, k, d):
        if k == half:
            zs[0, k - 1] = pack(total)
            for e in (0, 1):
                at = pl.ds(*cuts[e])
                wires.send(("z", e, k), zs.at[0, k - 1, :, at], zs_in.at[e, k - 1, :, at], along_z[e])
        elif k == half - 1:
            wires.arrived(("z", d, half), zs_in.at[d, half - 1, :, pl.ds(*cuts[d])], along_z[d])
            zs[d, k - 1] = pack(with_part(total, zs_in.at[d], half - 1, d))
            wires.send(("z", d, k), zs.at[d, k - 1], zs_in.at[d, k - 1], along_z[d])
        elif k > 0:
            wires.arrived(("z", d, k + 1), zs_in.at[d, k], along_z[d])
            zs[d, k - 1] = pack(total + zs_in[d, k].astype(jnp.float32))
            wires.send(("z", d, k), zs.at[d, k - 1], zs_in.at[d, k - 1], along_z[d])
        else:
            for e in (0, 1):
                wires.arrived(("z", e, 1), zs_in.at[e, 0], along_z[e])
                total = total + zs_in[e, 0].astype(jnp.float32)
            score = joined_score(total[:, -LANES:])
            out_ref[c] = jnp.concatenate([total[:, :-LANES], score], axis=1)
            wires.send("pair", out_ref.at[c], out_ref.at[c], partner)
            wires.arrived("pair", out_ref.at[1 - c], partner)

    for key in keys:
        s = slabs(key[0])[key[1]]
        wires.send(("d", key), part_ref.at[1 - c, s], other.at[s], partner)
    for k in range(half, -3, -1):
        for j, act in ((k, start_x), (k + 1, middle_x)):
            if 0 <= j <= half:
                for d, s in enumerate(slabs(j)):
                    act(s, (j, d))
        j = k + 2
        if 0 <= j <= half:
            for d, s in enumerate(slabs(j)):
                hop_z(end_x(s, (j, d)), j, d)
    wires.drain()


def reduce_rows(part):
    ring, line, rows, width = part.shape[1:]
    half = ring // 2
    wires = ring + 4 * ring + 2 * half + 1
    return pl.pallas_call(
        reduce_kernel,
        out_shape=jax.ShapeDtypeStruct((2, rows, width), jnp.float32),
        in_specs=[pl.BlockSpec(memory_space=pltpu.VMEM)],
        out_specs=pl.BlockSpec(memory_space=pltpu.VMEM),
        scratch_shapes=[
            pltpu.VMEM((ring, line, rows, width), part.dtype),
            pltpu.VMEM((ring, rows, width), part.dtype),
            pltpu.VMEM((ring, rows, width), part.dtype),
            pltpu.VMEM((2, ring, rows, width), part.dtype),
            pltpu.VMEM((2, ring, rows, width), part.dtype),
            pltpu.VMEM((2, half, rows, width), part.dtype),
            pltpu.VMEM((2, half, rows, width), part.dtype),
            pltpu.SemaphoreType.DMA((wires,)),
            pltpu.SemaphoreType.DMA((wires,)),
        ],
        compiler_params=pltpu.CompilerParams(collective_id=1, has_side_effects=True),
        name="reduce_rows",
    )(part)


def silu_parts(gate):
    sigma = jax.nn.sigmoid(gate)
    return (gate * sigma, sigma * (1.0 + gate * (1.0 - sigma)))


def contract(left, right, left_dim, right_dim):
    return lax.dot_general(
        left, right, (((left_dim,), (right_dim,)), ((), ())), preferred_element_type=jnp.float32
    )


def per_device(tokens, out_grad, expert_ids, probs, w_gate, w_up, w_down):
    ring, line = lax.axis_size("expert"), lax.axis_size("tensor")
    mine = lax.axis_index("expert") // (ring // EXPERTS)
    core = lax.axis_index("seq")
    count, width = tokens.shape
    lanes = jnp.arange(LANES, dtype=jnp.int32)
    named = expert_ids[:, :, None] == lanes[None, None, :]
    table = jnp.sum(
        jnp.where(named, probs[:, :, None].astype(jnp.float32), 0.0), axis=1
    ).astype(jnp.bfloat16)

    def placed(rows):
        part_a = width * 5 // 8 // LANES * LANES
        rows = jnp.concatenate([rows[:, :part_a], table, rows[:, part_a:]], axis=1)
        zero = jnp.zeros_like(rows)
        first, second = jnp.concatenate([rows, zero]), jnp.concatenate([zero, rows])
        return jnp.where(core == 0, first, second)

    wide = width * 5 // 8 // LANES * LANES + LANES
    x_all, dy_all, tables = gather_rows(jnp.stack([placed(tokens), placed(out_grad)]), wide)
    inputs, cotangent = x_all.reshape(-1, width), dy_all.reshape(-1, width)
    tables = tables.reshape(-1, LANES).astype(jnp.float32)
    scale = jnp.sum(jnp.where(lanes[None] == mine, tables, 0.0), axis=1)[:, None]
    w_g, w_u, w_d = w_gate[0], w_up[0], w_down[0]
    gate = jnp.dot(inputs, w_g, preferred_element_type=jnp.float32)
    up = jnp.dot(inputs, w_u, preferred_element_type=jnp.float32)
    back = contract(cotangent, w_d, 1, 1)
    act, slope = silu_parts(gate)
    hidden = act * up
    score = jnp.sum(back * hidden, axis=1)
    scaled = scale * back
    d_gate = (scaled * up * slope).astype(jnp.bfloat16)
    d_up = (scaled * act).astype(jnp.bfloat16)
    weighted = (scale * hidden).astype(jnp.bfloat16)
    part_dx = (contract(d_gate, w_g, 1, 1) + contract(d_up, w_u, 1, 1)).astype(jnp.bfloat16)
    part_score = jnp.where(lanes[None] % (LANES // 2) == mine, score[:, None], 0.0)
    high = lax.reduce_precision(part_score, 8, 7)
    part_score = jnp.where(lanes[None] < LANES // 2, high, part_score - high).astype(jnp.bfloat16)
    side = width // 2
    part = jnp.stack(
        [
            jnp.concatenate([part_dx[:, :side], part_score], axis=1),
            jnp.concatenate([part_dx[:, side:], part_score], axis=1),
        ]
    )
    total = reduce_rows(part.reshape(2, ring, line, -1, side + LANES))
    total = jnp.where(core == 0, total[:, :count], total[:, count:])
    grad_tokens = jnp.concatenate([total[0, :, :side], total[1, :, :side]], axis=1)
    grad_probs = jnp.sum(jnp.where(named, total[0, :, None, side:], 0.0), axis=2)
    grad_g = contract(inputs, d_gate, 0, 0).astype(jnp.bfloat16)[None]
    grad_u = contract(inputs, d_up, 0, 0).astype(jnp.bfloat16)[None]
    grad_d = contract(weighted, cotangent, 0, 0).astype(jnp.bfloat16)[None]
    return (grad_tokens, grad_probs, grad_g, grad_u, grad_d)


def solution(mesh):
    rows = P(("parts", "expert", "tensor", "seq"), None)
    return jax.shard_map(
        per_device,
        mesh=mesh,
        in_specs=(
            rows,
            rows,
            rows,
            rows,
            P("expert", None, ("tensor", "seq")),
            P("expert", None, ("tensor", "seq")),
            P("expert", ("tensor", "seq"), None),
        ),
        out_specs=(
            rows,
            rows,
            P(("parts", "expert"), None, ("tensor", "seq")),
            P(("parts", "expert"), None, ("tensor", "seq")),
            P(("parts", "expert"), ("tensor", "seq"), None),
        ),
        check_vma=False,
    )
```
